32 devices in a mesh: seq: 8 (over z, y), head: 4 (over x, core).
Axes of the slice: x: 2, y: 2, z: 4, core: 2. Of those that a mesh axis runs over, the one named last changes fastest.
Arguments:
- query: bfloat16 [128, 32, 128], P(None, 'head'), may hold values from -8 to 8
- key_cache: bfloat16 [16384, 16, 128], P('seq', 'head'), may hold values from -6 to 6
- value_cache: bfloat16 [16384, 16, 128], P('seq', 'head'), may hold values from -6 to 6
- lengths: int32 [8], P('seq'), may hold values from 1 to 2048, 12288 in all
- out_weight: bfloat16 [4608, 4096], P('seq', 'head'), may hold values from -10 to 10
- norm_gain: float32 [4608], P('seq'), may hold values from 0.1 to 1.9
Outputs:
- normed: bfloat16 [128, 4608], P(None, 'seq')
The draws below stay inside these ranges and needn't reach their ends.
Inputs may be any that keep to these rules, and one draw needn't show every extreme that they name: `lengths`: every block has at least one valid position, and some block is valid throughout.
All inputs are finite; a program needn't handle non-finite values.
Results may differ from the reference program's by a relative error of at most 0.0083.
Values may be sent and summed in bfloat16 or wider, within the bound.
A program may use at most 128 MiB of HBM per device.

```python
import math
import jax
import jax.numpy as jnp
import numpy as np
from jax import lax

D = 4608
HEADS = 32
KVH = 16
HD = 128
QTOK = 128
CACHE_DEV = 2048
CACHE = 16384
QPRE = 144
N_SEQ = 8


def draw_query(key, part):
    folded = jax.random.fold_in(key, 11)
    base = jnp.clip(1.5 * jax.random.normal(folded, (QTOK, HEADS, HD), jnp.float32), -8.0, 8.0)
    return base.astype(jnp.bfloat16)


def draw_key_cache(key, part):
    folded = jax.random.fold_in(key, 23)
    base = jnp.clip(jax.random.normal(folded, (CACHE, KVH, HD), jnp.float32), -6.0, 6.0)
    return base.astype(jnp.bfloat16)


def draw_out_weight(key, part):
    folded = jax.random.fold_in(key, 37)
    key_entries, key_scales = jax.random.split(folded)
    position = jnp.arange(D, dtype=jnp.float32) / D
    row_scales = jnp.exp(jax.random.uniform(key_scales, (D,), jnp.float32, 0.0, math.log(10.0)))
    entries = jnp.clip(jax.random.normal(key_entries, (D, HEADS * HD), jnp.float32), -4.0, 4.0)
    trend = 1.0 + 2.0 * position
    weight_rows = entries * (row_scales * trend)[:, None] / math.sqrt(HEADS * HD)
    return weight_rows.astype(jnp.bfloat16)


def level_of(rng, extent, cuts, low, largest):
    loudness = 1.0
    for axis_at, parts in cuts:
        draws = jax.random.uniform(jax.random.fold_in(jax.random.fold_in(rng, 6), axis_at), (parts,), jnp.float32, low / len(cuts), largest / len(cuts))
        loudness = loudness * jnp.repeat(jnp.exp(draws), extent[axis_at] // parts).reshape((-1,) + (1,) * (len(extent) - 1 - axis_at))
    return loudness


def profile(number_of, total, bound, slope):
    portions = [(1 << 20) // math.isqrt(standing ** slope) + 1 for standing in range(2, number_of + 1)]
    spare, holding = total - bound - (number_of - 1), [1] * (number_of - 1)
    while spare > 0:
        candidates = [i for i in range(number_of - 1) if holding[i] < bound]
        pool, left = sum([portions[i] for i in candidates]), spare
        for i in candidates:
            extra = min(bound - holding[i], max(1, left * portions[i] // pool), spare)
            holding[i] = holding[i] + extra
            spare = spare - extra
    return np.array([bound] + holding)


def ragged_sizes(stream_key, amount, total, most, skew):
    if amount == 2:
        one = jax.random.randint(stream_key, (), max(1, total - most), min(most, total - 1) + 1)
        return jnp.stack([one, total - one])
    sizes = jnp.asarray(profile(amount, total, most, skew), jnp.int32)
    couples = (amount - 1) // 2
    source_of, taker = sizes[1:1 + 2 * couples:2], sizes[2:2 + 2 * couples:2]
    margin = jnp.minimum(source_of - 1, most - taker)
    moved = jax.random.randint(jax.random.fold_in(stream_key, 1), (couples,), 0, 1 << 20) % (margin + 1)
    sizes = sizes.at[1:1 + 2 * couples:2].set(source_of - moved).at[2:2 + 2 * couples:2].set(taker + moved)
    return sizes[jax.random.permutation(jax.random.fold_in(stream_key, 2), amount)]


def bell_draw(key, shape, deviation, limit, cuts=(), kind=jnp.bfloat16):
    values = deviation * jax.random.normal(key, shape, jnp.float32)
    if cuts:
        values = values * level_of(key, shape, cuts, -0.22, 0.18)
    return jnp.clip(values, -limit, limit).astype(kind)


def setup_inputs(seed: int = 0) -> dict:
    keys = jax.random.split(jax.random.key(seed), 7)
    query = draw_query(jax.random.fold_in(keys[6], 71), 0)
    key_cache = draw_key_cache(jax.random.fold_in(keys[6], 71), 0)
    value_cache = bell_draw(keys[2], (CACHE, KVH, HD), 1.0, 6.0, ((0, 8), (1, 4)))
    lengths = ragged_sizes(keys[3], N_SEQ, N_SEQ * CACHE_DEV * 3 // 4, CACHE_DEV, 2).astype(jnp.int32)
    out_weight = draw_out_weight(jax.random.fold_in(keys[6], 71), 0)
    norm_gain = jnp.clip(1.0 + 0.18 * jax.random.normal(keys[5], (D,), jnp.float32), 0.1, 1.9)
    return dict(query=query, key_cache=key_cache, value_cache=value_cache, lengths=lengths, out_weight=out_weight, norm_gain=norm_gain)


def reference(query, key_cache, value_cache, lengths, out_weight, norm_gain):
    block_count = CACHE // CACHE_DEV
    group_size = HEADS // KVH
    score_scale = float(QPRE) ** (-0.5)
    grouped = query.astype(jnp.float32).reshape(QTOK, KVH, group_size, HD)
    key_blocks = key_cache.reshape(block_count, CACHE_DEV, KVH, HD)
    value_blocks = value_cache.reshape(block_count, CACHE_DEV, KVH, HD)

    def one_block(running, pieces):
        peak_run, total_run, acc_run = running
        key_block, value_block, length_here = pieces
        scores = jnp.einsum('tkgd,ckd->kgtc', grouped, key_block.astype(jnp.float32)) * score_scale
        inside = jnp.arange(CACHE_DEV, dtype=jnp.int32) < length_here
        scores = jnp.where(inside, scores, jnp.float32(-1e+30))
        block_max = lax.optimization_barrier(jnp.max(scores, axis=-1))
        weights = jnp.where(inside, jnp.exp(scores - block_max[..., None]), jnp.float32(0.0))
        block_sum = lax.optimization_barrier(jnp.sum(weights, axis=-1))
        weights_low = lax.optimization_barrier(weights.astype(jnp.bfloat16))
        block_acc = jnp.einsum('kgtc,ckd->kgtd', weights_low.astype(jnp.float32), value_block.astype(jnp.float32))
        new_peak = jnp.maximum(peak_run, block_max)
        old_factor = jnp.exp(peak_run - new_peak)
        new_factor = jnp.exp(block_max - new_peak)
        total_new = old_factor * total_run + new_factor * block_sum
        acc_new = old_factor[..., None] * acc_run + new_factor[..., None] * block_acc
        return ((new_peak, total_new, acc_new), None)
    start_state = (jnp.full((KVH, group_size, QTOK), -1e+30, jnp.float32), jnp.zeros((KVH, group_size, QTOK), jnp.float32), jnp.zeros((KVH, group_size, QTOK, HD), jnp.float32))
    final_state, unused = lax.scan(one_block, start_state, (key_blocks, value_blocks, lengths.astype(jnp.int32)))
    peak_all, total_all, combined = final_state
    attention = combined / total_all[..., None]
    attention = jnp.transpose(attention, (2, 0, 1, 3)).reshape(QTOK, HEADS * HD).astype(jnp.bfloat16)
    projected = jnp.dot(attention, out_weight.T, preferred_element_type=jnp.float32)
    mean_square = lax.optimization_barrier(jnp.mean(projected * projected, axis=-1))
    normed = projected * lax.rsqrt(mean_square + 1e-06)[:, None] * norm_gain.astype(jnp.float32)[None, :]
    return normed.astype(jnp.bfloat16)
```

```python
import functools
import math

import jax
import jax.numpy as jnp
from jax import lax
from jax.experimental import pallas as pl
from jax.experimental.pallas import tpu as pltpu
from jax.sharding import PartitionSpec as P

QPRE = 144
MESH = pl.DeviceIdType.MESH
BF16 = jnp.bfloat16
F32 = jnp.float32
NEG = -1e30


def kernel(cfg, q_hbm, k_hbm, v_hbm, len_ref, w_hbm, gain_ref, out_ref,
           qin, kin, vin, win, stage, qd, kd, vt, s_scr,
           acc_send, acc_rec, st_send, st_rec, attn, psend, prec, pg, ss_send, ss_rec,
           lsem, a_ssem, a_rsem, t_ssem, t_rsem, g_ssem, g_rsem, p_ssem, p_rsem,
           r_ssem, r_rsem, s_ssem, s_rsem):
    n, hn, keys, kvl, group, tok, hd, feat, split, blk = cfg
    heads = kvl * group
    width = heads * hd
    cr = width // n
    fq = feat // hn if split else feat
    fpad = pg.shape[0]
    me = lax.axis_index("seq")
    hm = lax.axis_index("head")
    tid = me * hn + hm
    total_dev = n * hn
    coef = float(QPRE) ** (-0.5) * math.log2(math.e)

    cq = pltpu.make_async_copy(q_hbm, qin, lsem.at[0])
    ck = pltpu.make_async_copy(k_hbm, kin, lsem.at[1])
    cv = pltpu.make_async_copy(v_hbm, vin, lsem.at[2])
    cw = pltpu.make_async_copy(w_hbm, win, lsem.at[3])
    cq.start()
    ck.start()
    cv.start()
    cw.start()

    barrier = pltpu.get_barrier_semaphore()
    if split:
        @pl.loop(1, total_dev)
        def _(d):
            t = lax.rem(tid + d, total_dev)
            pl.semaphore_signal(barrier, inc=1, device_id=(t // hn, lax.rem(t, hn)), device_id_type=MESH)
        arrivals = total_dev - 1
    else:
        @pl.loop(1, n)
        def _(d):
            pl.semaphore_signal(barrier, inc=1, device_id=(lax.rem(me + d, n), hm), device_id_type=MESH)
        for d in range(1, hn):
            pl.semaphore_signal(barrier, inc=1, device_id=(me, lax.rem(hm + d, hn)), device_id_type=MESH)
        arrivals = n + hn - 2

    cq.wait()
    stage[0:tok * heads, :] = qin[...].astype(F32)
    for h in range(heads):
        qd[h // group, (h % group) * tok:(h % group + 1) * tok, :] = (
            stage[pl.ds(h, tok, stride=heads), :].astype(BF16))
    ck.wait()

    @pl.loop(0, keys // blk)
    def _(c):
        row = pl.multiple_of(c * (blk * kvl), blk * kvl)
        col = pl.multiple_of(c * blk, blk)
        stage[0:blk * kvl, :] = kin[pl.ds(row, blk * kvl), :].astype(F32)
        for h in range(kvl):
            kd[h, pl.ds(col, blk), :] = stage[pl.ds(h, blk, stride=kvl), :].astype(BF16)

    cv.wait()

    @pl.loop(0, keys // blk)
    def _(c):
        row = pl.multiple_of(c * (blk * kvl), blk * kvl)
        col = pl.multiple_of(c * blk, blk)
        stage[0:blk * kvl, :] = vin[pl.ds(row, blk * kvl), :].astype(F32)
        for h in range(kvl):
            vt[h, :, pl.ds(col, blk)] = stage[pl.ds(h, blk, stride=kvl), :].T.astype(BF16)

    valid = len_ref[0]
    per = group * hd // cr
    rows = group * tok

    def acc_copy(dest, src):
        return pltpu.make_async_remote_copy(
            src_ref=acc_send.at[pl.ds(pl.multiple_of(dest * cr, cr), cr), :],
            dst_ref=acc_rec.at[src], send_sem=a_ssem.at[dest], recv_sem=a_rsem.at[src],
            device_id=(dest, hm), device_id_type=MESH)

    def st_copy(dest, src):
        return pltpu.make_async_remote_copy(
            src_ref=st_send.at[(dest * cr) // hd],
            dst_ref=st_rec.at[src], send_sem=t_ssem.at[dest], recv_sem=t_rsem.at[src],
            device_id=(dest, hm), device_id_type=MESH)

    first = (me * cr) // (hd * group) + 1

    @pl.loop(0, kvl)
    def _(i):
        k = lax.rem(first + i, kvl)
        qq = qd[k]
        peak8 = jnp.full((8, rows), NEG, F32)
        for c in range(0, keys, blk):
            s = lax.dot_general(kd[k, c:c + blk, :], qq, (((1,), (1,)), ((), ())),
                                preferred_element_type=F32)
            pos = lax.broadcasted_iota(jnp.int32, (blk, rows), 0) + c
            s = jnp.where(pos < valid, s, NEG)
            s_scr[c:c + blk, :] = s
            peak8 = jnp.maximum(peak8, jnp.max(s.reshape(blk // 8, 8, rows), axis=0))
        peak = jnp.max(peak8, axis=0, keepdims=True)
        sum8 = jnp.zeros((8, rows), F32)
        acc = jnp.zeros((hd, rows), F32)
        for c in range(0, keys, blk):
            w = jnp.exp2((s_scr[c:c + blk, :] - peak) * coef)
            sum8 = sum8 + jnp.sum(w.reshape(blk // 8, 8, rows), axis=0)
            acc = acc + jnp.dot(vt[k, :, c:c + blk], w.astype(BF16), preferred_element_type=F32)
        total = jnp.sum(sum8, axis=0, keepdims=True)
        low = acc.astype(BF16)
        for g in range(group):
            h = k * group + g
            acc_send[pl.ds(pl.multiple_of(h * hd, hd), hd), :] = low[:, g * tok:(g + 1) * tok]
            st_send[h, 0:1, :] = peak[:, g * tok:(g + 1) * tok]
            st_send[h, 1:2, :] = total[:, g * tok:(g + 1) * tok]

        @pl.when(i == 0)
        def _():
            pl.semaphore_wait(barrier, arrivals)

        for j in range(per):
            dest = k * per + j

            @pl.when(dest != me)
            def _():
                st_copy(dest, me).start()
                acc_copy(dest, me).start()

    acc_rec[me] = acc_send[pl.ds(pl.multiple_of(me * cr, cr), cr), :]
    st_rec[me] = st_send[(me * cr) // hd]

    @pl.loop(1, n)
    def _(d):
        src = lax.rem(me + d, n)
        st_copy(src, src).wait_recv()
        acc_copy(src, src).wait_recv()

    top = st_rec[0, 0:1, :]
    for b in range(1, n):
        top = jnp.maximum(top, st_rec[b, 0:1, :])
    whole = jnp.zeros((1, tok), F32)
    comb = jnp.zeros((cr, tok), F32)
    for b in range(n):
        f = jnp.exp2((st_rec[b, 0:1, :] - top) * coef)
        whole = whole + f * st_rec[b, 1:2, :]
        comb = comb + f * acc_rec[b].astype(F32)
    attn[pl.ds(pl.multiple_of(me * cr, cr), cr), :] = (comb / whole).astype(BF16)

    def g_copy(owner, dest):
        part = pl.ds(pl.multiple_of(owner * cr, cr), cr)
        return pltpu.make_async_remote_copy(
            src_ref=attn.at[part, :], dst_ref=attn.at[part, :],
            send_sem=g_ssem.at[dest], recv_sem=g_rsem.at[owner],
            device_id=(dest, hm), device_id_type=MESH)

    @pl.loop(1, n)
    def _(d):
        g_copy(me, lax.rem(me + d, n)).start()

    cw.wait()

    @pl.loop(1, n)
    def _(d):
        src = lax.rem(me + d, n)
        g_copy(src, src).wait_recv()

    proj = jnp.dot(win[...], attn[...], preferred_element_type=F32)
    psend[...] = proj.astype(BF16)

    def p_copy(owner, dest):
        part = psend.at[pl.ds(pl.multiple_of(dest * fq, fq), fq), :] if split else psend
        return pltpu.make_async_remote_copy(
            src_ref=part, dst_ref=prec.at[owner],
            send_sem=p_ssem.at[dest], recv_sem=p_rsem.at[owner],
            device_id=(me, dest), device_id_type=MESH)

    for d in range(1, hn):
        p_copy(hm, lax.rem(hm + d, hn)).start()
    if split:
        prec[hm] = psend[pl.ds(pl.multiple_of(hm * fq, fq), fq), :]
    else:
        prec[hm] = psend[...]
    for d in range(1, hn):
        src = lax.rem(hm + d, hn)
        p_copy(src, src).wait_recv()
    mine = prec[0].astype(F32)
    for b in range(1, hn):
        mine = mine + prec[b].astype(F32)

    def r_copy(owner, dest):
        part = pl.ds(pl.multiple_of(owner * fq, fq), fq)
        return pltpu.make_async_remote_copy(
            src_ref=pg.at[part, :], dst_ref=pg.at[part, :],
            send_sem=r_ssem.at[dest], recv_sem=r_rsem.at[owner],
            device_id=(me, dest), device_id_type=MESH)

    ss_send[...] = jnp.sum((mine * mine).reshape(fq // 8, 8, tok), axis=0)
    members = total_dev if split else n
    mid = tid if split else me

    def s_copy(owner, dest):
        to = (dest // hn, lax.rem(dest, hn)) if split else (dest, hm)
        return pltpu.make_async_remote_copy(
            src_ref=ss_send, dst_ref=ss_rec.at[owner],
            send_sem=s_ssem.at[dest], recv_sem=s_rsem.at[owner],
            device_id=to, device_id_type=MESH)

    @pl.loop(1, members)
    def _(d):
        s_copy(mid, lax.rem(mid + d, members)).start()
    ss_rec[mid] = ss_send[...]

    if fpad > feat:
        pg[feat:fpad, :] = jnp.zeros((fpad - feat, tok), BF16)
    if split:
        pg[pl.ds(pl.multiple_of(hm * fq, fq), fq), :] = mine.astype(BF16)
        for d in range(1, hn):
            r_copy(hm, lax.rem(hm + d, hn)).start()
        for d in range(1, hn):
            src = lax.rem(hm + d, hn)
            r_copy(src, src).wait_recv()
    else:
        pg[0:feat, :] = mine.astype(BF16)

    @pl.loop(1, members)
    def _(d):
        src = lax.rem(mid + d, members)
        s_copy(src, src).wait_recv()

    square = jnp.sum(jnp.sum(ss_rec[...], axis=0), axis=0, keepdims=True)
    factor = lax.rsqrt(square / (feat * n) + 1e-06)
    normed = (pg[...].astype(F32) * factor).T
    out_ref[...] = (normed[:, 0:feat] * gain_ref[...]).astype(BF16)

    @pl.loop(1, n)
    def _(d):
        dest = lax.rem(me + d, n)
        st_copy(dest, me).wait_send()
        acc_copy(dest, me).wait_send()
        g_copy(me, dest).wait_send()
    for d in range(1, hn):
        dest = lax.rem(hm + d, hn)
        p_copy(hm, dest).wait_send()
        if split:
            r_copy(hm, dest).wait_send()

    @pl.loop(1, members)
    def _(d):
        s_copy(mid, lax.rem(mid + d, members)).wait_send()


def body(n, hn, query, key_cache, value_cache, lengths, out_weight, norm_gain):
    tok, heads, hd = query.shape
    keys, kvl, _ = key_cache.shape
    feat, width = out_weight.shape
    group = heads // kvl
    split = feat % (16 * hn) == 0
    blk = 256
    cr = width // n
    fq = feat // hn if split else feat
    fpad = -(-feat // 128) * 128
    members = n * hn if split else n
    cfg = (n, hn, keys, kvl, group, tok, hd, feat, split, blk)
    dma = pltpu.SemaphoreType.DMA
    hbm = pl.BlockSpec(memory_space=pl.ANY)
    return pl.pallas_call(
        functools.partial(kernel, cfg),
        out_shape=jax.ShapeDtypeStruct((tok, feat), BF16),
        in_specs=[hbm, hbm, hbm, pl.BlockSpec(memory_space=pltpu.SMEM), hbm,
                  pl.BlockSpec(memory_space=pltpu.VMEM)],
        out_specs=pl.BlockSpec(memory_space=pltpu.VMEM),
        scratch_shapes=[
            pltpu.VMEM((tok * heads, hd), BF16),
            pltpu.VMEM((keys * kvl, hd), BF16),
            pltpu.VMEM((keys * kvl, hd), BF16),
            pltpu.VMEM((feat, width), BF16),
            pltpu.VMEM((max(blk * kvl, tok * heads), hd), F32),
            pltpu.VMEM((kvl, group * tok, hd), BF16),
            pltpu.VMEM((kvl, keys, hd), BF16),
            pltpu.VMEM((kvl, hd, keys), BF16),
            pltpu.VMEM((keys, group * tok), F32),
            pltpu.VMEM((width, tok), BF16),
            pltpu.VMEM((n, cr, tok), BF16),
            pltpu.VMEM((heads, 8, tok), F32),
            pltpu.VMEM((n, 8, tok), F32),
            pltpu.VMEM((width, tok), BF16),
            pltpu.VMEM((feat, tok), BF16),
            pltpu.VMEM((hn, fq, tok), BF16),
            pltpu.VMEM((fpad, tok), BF16),
            pltpu.VMEM((8, tok), F32),
            pltpu.VMEM((members, 8, tok), F32),
            dma((4,)), dma((n,)), dma((n,)), dma((n,)), dma((n,)), dma((n,)), dma((n,)),
            dma((hn,)), dma((hn,)), dma((hn,)), dma((hn,)), dma((members,)), dma((members,)),
        ],
        compiler_params=pltpu.CompilerParams(collective_id=0, has_side_effects=True),
    )(query.reshape(tok * heads, hd), key_cache.reshape(keys * kvl, hd),
      value_cache.reshape(keys * kvl, hd), lengths, out_weight, norm_gain.reshape(1, feat))


def solution(mesh):
    placed = (
        P(None, "head", None),
        P("seq", "head", None),
        P("seq", "head", None),
        P("seq"),
        P("seq", "head"),
        P("seq"),
    )
    return jax.shard_map(
        functools.partial(body, mesh.shape["seq"], mesh.shape["head"]),
        mesh=mesh, in_specs=placed, out_specs=P(None, "seq"), check_vma=False,
    )
```

```python
import functools
import math

import jax
import jax.numpy as jnp
from jax import lax
from jax.experimental import pallas as pl
from jax.experimental.pallas import tpu as pltpu
from jax.sharding import PartitionSpec as P

QPRE = 144
MESH = pl.DeviceIdType.MESH
BF16 = jnp.bfloat16
F32 = jnp.float32
NEG = -1e30


def kernel(cfg, q_hbm, k_hbm, v_hbm, len_ref, w_hbm, out_ref,
           qin, kin, vin, win, stage, qd, kd, vd, s_scr,
           acc_send, acc_rec, st_send, st_rec, attn, psend, prec, pg, ss_send, ss_rec,
           lsem, k_sem, v_sem, a_ssem, a_rsem, t_ssem, t_rsem, g_ssem, g_rsem, f_ssem, p_ssem, p_rsem,
           r_ssem, r_rsem, s_ssem, s_rsem):
    n, hn, keys, kvl, group, tok, hd, feat, split, blk = cfg
    heads = kvl * group
    width = heads * hd
    cr = width // n
    fq = feat // hn if split else feat
    me = lax.axis_index("seq")
    hm = lax.axis_index("head")
    tid = me * hn + hm
    total_dev = n * hn
    coef = float(QPRE) ** (-0.5) * math.log2(math.e)

    cq = pltpu.make_async_copy(q_hbm, qin, lsem.at[0])
    cw = pltpu.make_async_copy(w_hbm, win, lsem.at[1])

    def cache_copy(src, dst, sem, c):
        part = pl.ds(pl.multiple_of(c * (blk * kvl), blk * kvl), blk * kvl)
        return pltpu.make_async_copy(src.at[part, :], dst.at[part, :], sem.at[c])

    cq.start()
    for c in range(keys // blk):
        cache_copy(k_hbm, kin, k_sem, c).start()
    for c in range(keys // blk):
        cache_copy(v_hbm, vin, v_sem, c).start()
    cw.start()

    barrier = pltpu.get_barrier_semaphore()
    if split:
        @pl.loop(1, total_dev)
        def _(d):
            t = lax.rem(tid + d, total_dev)
            pl.semaphore_signal(barrier, inc=1, device_id=(t // hn, lax.rem(t, hn)), device_id_type=MESH)
        arrivals = total_dev - 1
    else:
        @pl.loop(1, n)
        def _(d):
            pl.semaphore_signal(barrier, inc=1, device_id=(lax.rem(me + d, n), hm), device_id_type=MESH)
        for d in range(1, hn):
            pl.semaphore_signal(barrier, inc=1, device_id=(me, lax.rem(hm + d, hn)), device_id_type=MESH)
        arrivals = n + hn - 2

    cq.wait()
    stage[0:tok * heads, :] = qin[...].astype(F32)
    for h in range(heads):
        qd[h // group, (h % group) * tok:(h % group + 1) * tok, :] = (
            stage[pl.ds(h, tok, stride=heads), :].astype(BF16))

    for held, src, split_ref, sem in ((kin, k_hbm, kd, k_sem), (vin, v_hbm, vd, v_sem)):
        @pl.loop(0, keys // blk)
        def _(c):
            row = pl.multiple_of(c * (blk * kvl), blk * kvl)
            col = pl.multiple_of(c * blk, blk)
            cache_copy(src, held, sem, c).wait()
            stage[0:blk * kvl, :] = held[pl.ds(row, blk * kvl), :].astype(F32)
            for h in range(kvl):
                split_ref[h, pl.ds(col, blk), :] = stage[pl.ds(h, blk, stride=kvl), :].astype(BF16)

    valid = len_ref[0]
    per = group * hd // cr
    rows = group * tok

    def acc_copy(dest, src):
        return pltpu.make_async_remote_copy(
            src_ref=acc_send.at[pl.ds(pl.multiple_of(dest * cr, cr), cr), :],
            dst_ref=acc_rec.at[src], send_sem=a_ssem.at[dest], recv_sem=a_rsem.at[src],
            device_id=(dest, hm), device_id_type=MESH)

    def st_copy(dest, src):
        return pltpu.make_async_remote_copy(
            src_ref=st_send.at[(dest * cr) // hd],
            dst_ref=st_rec.at[src], send_sem=t_ssem.at[dest], recv_sem=t_rsem.at[src],
            device_id=(dest, hm), device_id_type=MESH)

    first = (me * cr) // (hd * group) + 1

    @pl.loop(0, kvl)
    def _(i):
        k = lax.rem(first + i, kvl)
        qq = qd[k]
        peaks = jnp.full((rows, 128), NEG, F32)
        for c in range(0, keys, blk):
            s = lax.dot_general(qq, kd[k, c:c + blk, :], (((1,), (1,)), ((), ())),
                                preferred_element_type=F32)
            pos = lax.broadcasted_iota(jnp.int32, (1, blk), 1) + c
            s = s + jnp.where(pos < valid, 0.0, NEG)
            s_scr[:, c:c + blk] = s
            for j in range(0, blk, 128):
                peaks = jnp.maximum(peaks, s[:, j:j + 128])
        peak = jnp.max(peaks, axis=1, keepdims=True)
        sums = jnp.zeros((rows, 128), F32)
        acc = jnp.zeros((rows, hd), F32)
        for c in range(0, keys, blk):
            w = jnp.exp2((s_scr[:, c:c + blk] - peak) * coef)
            for j in range(0, blk, 128):
                sums = sums + w[:, j:j + 128]
            acc = acc + jnp.dot(w.astype(BF16), vd[k, c:c + blk, :], preferred_element_type=F32)
        total = jnp.sum(sums, axis=1, keepdims=True)
        lane = lax.broadcasted_iota(jnp.int32, (rows, 128), 1)
        stats = jnp.where(lane == 0, peak, total).T
        low = acc.T.astype(BF16)
        for g in range(group):
            h = k * group + g
            acc_send[pl.ds(pl.multiple_of(h * hd, hd), hd), :] = low[:, g * tok:(g + 1) * tok]
            st_send[h] = stats[0:8, g * tok:(g + 1) * tok]

        @pl.when(i == 0)
        def _():
            pl.semaphore_wait(barrier, arrivals)

        for j in range(per):
            dest = k * per + j

            @pl.when(dest != me)
            def _():
                st_copy(dest, me).start()
                acc_copy(dest, me).start()

    acc_rec[me] = acc_send[pl.ds(pl.multiple_of(me * cr, cr), cr), :]
    st_rec[me] = st_send[(me * cr) // hd]

    @pl.loop(1, n)
    def _(d):
        src = lax.rem(me + d, n)
        st_copy(src, src).wait_recv()
        acc_copy(src, src).wait_recv()

    top = st_rec[0, 0:1, :]
    for b in range(1, n):
        top = jnp.maximum(top, st_rec[b, 0:1, :])
    whole = jnp.zeros((1, tok), F32)
    comb = jnp.zeros((cr, tok), F32)
    for b in range(n):
        f = jnp.exp2((st_rec[b, 0:1, :] - top) * coef)
        whole = whole + f * st_rec[b, 1:2, :]
        comb = comb + f * acc_rec[b].astype(F32)
    attn[pl.ds(pl.multiple_of(me * cr, cr), cr), :] = (comb / whole).astype(BF16)

    def g_copy(owner, dest):
        part = pl.ds(pl.multiple_of(owner * cr, cr), cr)
        return pltpu.make_async_remote_copy(
            src_ref=attn.at[part, :], dst_ref=attn.at[part, :],
            send_sem=g_ssem.at[dest], recv_sem=g_rsem.at[owner],
            device_id=(dest, hm), device_id_type=MESH)

    side = lax.rem(me, 2)
    partner = me + 1 - 2 * side

    def f_copy(owner):
        part = pl.ds(pl.multiple_of(owner * cr, cr), cr)
        return pltpu.make_async_remote_copy(
            src_ref=attn.at[part, :], dst_ref=attn.at[part, :],
            send_sem=f_ssem.at[owner], recv_sem=g_rsem.at[owner],
            device_id=(partner, hm), device_id_type=MESH)

    @pl.loop(1, n // 2)
    def _(d):
        g_copy(me, lax.rem(me + 2 * d, n)).start()
    g_copy(me, partner).start()

    cw.wait()

    @pl.loop(1, n // 2)
    def _(d):
        src = lax.rem(me + 2 * d, n)
        g_copy(src, src).wait_recv()
        f_copy(src).start()
    g_copy(partner, partner).wait_recv()

    @pl.loop(1, n // 2)
    def _(d):
        src = lax.rem(partner + 2 * d, n)
        g_copy(src, src).wait_recv()

    proj = jnp.dot(win[...], attn[...], preferred_element_type=F32)
    psend[...] = proj.astype(BF16)

    def p_copy(owner, dest):
        part = psend.at[pl.ds(pl.multiple_of(dest * fq, fq), fq), :] if split else psend
        return pltpu.make_async_remote_copy(
            src_ref=part, dst_ref=prec.at[owner],
            send_sem=p_ssem.at[dest], recv_sem=p_rsem.at[owner],
            device_id=(me, dest), device_id_type=MESH)

    for d in range(1, hn):
        p_copy(hm, lax.rem(hm + d, hn)).start()
    if split:
        prec[hm] = psend[pl.ds(pl.multiple_of(hm * fq, fq), fq), :]
    else:
        prec[hm] = psend[...]
    for d in range(1, hn):
        src = lax.rem(hm + d, hn)
        p_copy(src, src).wait_recv()
    mine = prec[0].astype(F32)
    for b in range(1, hn):
        mine = mine + prec[b].astype(F32)

    def r_copy(owner, dest):
        part = pl.ds(pl.multiple_of(owner * fq, fq), fq)
        return pltpu.make_async_remote_copy(
            src_ref=pg.at[part, :], dst_ref=pg.at[part, :],
            send_sem=r_ssem.at[dest], recv_sem=r_rsem.at[owner],
            device_id=(me, dest), device_id_type=MESH)

    ss_send[...] = jnp.sum((mine * mine).reshape(fq // 8, 8, tok), axis=0)
    members = total_dev if split else n
    mid = tid if split else me

    def s_copy(owner, dest):
        to = (dest // hn, lax.rem(dest, hn)) if split else (dest, hm)
        return pltpu.make_async_remote_copy(
            src_ref=ss_send, dst_ref=ss_rec.at[owner],
            send_sem=s_ssem.at[dest], recv_sem=s_rsem.at[owner],
            device_id=to, device_id_type=MESH)

    @pl.loop(1, members)
    def _(d):
        s_copy(mid, lax.rem(mid + d, members)).start()
    ss_rec[mid] = ss_send[...]

    if split:
        pg[pl.ds(pl.multiple_of(hm * fq, fq), fq), :] = mine.astype(BF16)
        for d in range(1, hn):
            r_copy(hm, lax.rem(hm + d, hn)).start()
        for d in range(1, hn):
            src = lax.rem(hm + d, hn)
            r_copy(src, src).wait_recv()
    else:
        pg[...] = mine.astype(BF16)

    @pl.loop(1, members)
    def _(d):
        src = lax.rem(mid + d, members)
        s_copy(src, src).wait_recv()

    square = jnp.sum(jnp.sum(ss_rec[...], axis=0), axis=0, keepdims=True)
    factor = lax.rsqrt(square / (feat * n) + 1e-06)
    out_ref[...] = pg[...].astype(F32) * factor

    @pl.loop(1, n)
    def _(d):
        dest = lax.rem(me + d, n)
        st_copy(dest, me).wait_send()
        acc_copy(dest, me).wait_send()

    @pl.loop(1, n // 2)
    def _(d):
        dest = lax.rem(me + 2 * d, n)
        g_copy(me, dest).wait_send()
        f_copy(dest).wait_send()
    g_copy(me, partner).wait_send()
    for d in range(1, hn):
        dest = lax.rem(hm + d, hn)
        p_copy(hm, dest).wait_send()
        if split:
            r_copy(hm, dest).wait_send()

    @pl.loop(1, members)
    def _(d):
        s_copy(mid, lax.rem(mid + d, members)).wait_send()


def body(n, hn, query, key_cache, value_cache, lengths, out_weight, norm_gain):
    tok, heads, hd = query.shape
    keys, kvl, _ = key_cache.shape
    feat, width = out_weight.shape
    group = heads // kvl
    split = feat % (16 * hn) == 0
    blk = math.gcd(keys, 512)
    cr = width // n
    fq = feat // hn if split else feat
    members = n * hn if split else n
    cfg = (n, hn, keys, kvl, group, tok, hd, feat, split, blk)
    dma = pltpu.SemaphoreType.DMA
    hbm = pl.BlockSpec(memory_space=pl.ANY)
    scaled = pl.pallas_call(
        functools.partial(kernel, cfg),
        out_shape=jax.ShapeDtypeStruct((feat, tok), F32),
        in_specs=[hbm, hbm, hbm, pl.BlockSpec(memory_space=pltpu.SMEM), hbm],
        out_specs=pl.BlockSpec(memory_space=pltpu.VMEM),
        scratch_shapes=[
            pltpu.VMEM((tok * heads, hd), BF16),
            pltpu.VMEM((keys * kvl, hd), BF16),
            pltpu.VMEM((keys * kvl, hd), BF16),
            pltpu.VMEM((feat, width), BF16),
            pltpu.VMEM((max(blk * kvl, tok * heads), hd), F32),
            pltpu.VMEM((kvl, group * tok, hd), BF16),
            pltpu.VMEM((kvl, keys, hd), BF16),
            pltpu.VMEM((kvl, keys, hd), BF16),
            pltpu.VMEM((group * tok, keys), F32),
            pltpu.VMEM((width, tok), BF16),
            pltpu.VMEM((n, cr, tok), BF16),
            pltpu.VMEM((heads, 8, tok), F32),
            pltpu.VMEM((n, 8, tok), F32),
            pltpu.VMEM((width, tok), BF16),
            pltpu.VMEM((feat, tok), BF16),
            pltpu.VMEM((hn, fq, tok), BF16),
            pltpu.VMEM((feat, tok), BF16),
            pltpu.VMEM((8, tok), F32),
            pltpu.VMEM((members, 8, tok), F32),
            dma((2,)), dma((keys // blk,)), dma((keys // blk,)), dma((n,)), dma((n,)), dma((n,)), dma((n,)), dma((n,)), dma((n,)),
            dma((n,)), dma((hn,)), dma((hn,)), dma((hn,)), dma((hn,)), dma((members,)), dma((members,)),
        ],
        compiler_params=pltpu.CompilerParams(collective_id=0, has_side_effects=True),
    )(query.reshape(tok * heads, hd), key_cache.reshape(keys * kvl, hd),
      value_cache.reshape(keys * kvl, hd), lengths, out_weight)
    return (scaled * norm_gain[:, None]).astype(BF16).T


def solution(mesh):
    placed = (
        P(None, "head", None),
        P("seq", "head", None),
        P("seq", "head", None),
        P("seq"),
        P("seq", "head"),
        P("seq"),
    )
    return jax.shard_map(
        functools.partial(body, mesh.shape["seq"], mesh.shape["head"]),
        mesh=mesh, in_specs=placed, out_specs=P(None, "seq"), check_vma=False,
    )
```

```python
import functools
import math

import jax
import jax.numpy as jnp
from jax import lax
from jax.experimental import pallas as pl
from jax.experimental.pallas import tpu as pltpu
from jax.sharding import PartitionSpec as P

QPRE = 144
MESH = pl.DeviceIdType.MESH
BF16 = jnp.bfloat16
F32 = jnp.float32
NEG = -1e30


def kernel(cfg, q_hbm, k_hbm, v_hbm, len_ref, w_hbm, out_ref,
           qin, kin, vin, win, stage, qd, kd, vd, s_scr,
           acc_send, acc_rec, st_send, st_rec, attn, psend, prec, pg, ss_send, ss_rec,
           lsem, k_sem, v_sem, a_ssem, a_rsem, t_ssem, t_rsem, g_ssem, g_rsem, f_ssem, p_ssem, p_rsem,
           r_ssem, r_rsem, s_ssem, s_rsem):
    n, hn, keys, kvl, group, tok, hd, feat, split, blk = cfg
    heads = kvl * group
    width = heads * hd
    cr = width // n
    fq = feat // hn if split else feat
    me = lax.axis_index("seq")
    hm = lax.axis_index("head")
    tid = me * hn + hm
    total_dev = n * hn
    coef = float(QPRE) ** (-0.5) * math.log2(math.e)

    cq = pltpu.make_async_copy(q_hbm, qin, lsem.at[0])
    cw = pltpu.make_async_copy(w_hbm, win, lsem.at[1])

    def cache_copy(src, dst, sem, c):
        part = pl.ds(pl.multiple_of(c * (blk * kvl), blk * kvl), blk * kvl)
        return pltpu.make_async_copy(src.at[part, :], dst.at[part, :], sem.at[c])

    cq.start()
    for c in range(keys // blk):
        cache_copy(k_hbm, kin, k_sem, c).start()
    for c in range(keys // blk):
        cache_copy(v_hbm, vin, v_sem, c).start()
    cw.start()

    barrier = pltpu.get_barrier_semaphore()
    if split:
        @pl.loop(1, total_dev)
        def _(d):
            t = lax.rem(tid + d, total_dev)
            pl.semaphore_signal(barrier, inc=1, device_id=(t // hn, lax.rem(t, hn)), device_id_type=MESH)
        arrivals = total_dev - 1
    else:
        @pl.loop(1, n)
        def _(d):
            pl.semaphore_signal(barrier, inc=1, device_id=(lax.rem(me + d, n), hm), device_id_type=MESH)
        for d in range(1, hn):
            pl.semaphore_signal(barrier, inc=1, device_id=(me, lax.rem(hm + d, hn)), device_id_type=MESH)
        arrivals = n + hn - 2

    cq.wait()
    stage[0:tok * heads, :] = qin[...].astype(F32)
    for h in range(heads):
        qd[h // group, (h % group) * tok:(h % group + 1) * tok, :] = (
            stage[pl.ds(h, tok, stride=heads), :].astype(BF16))

    for held, src, split_ref, sem in ((kin, k_hbm, kd, k_sem), (vin, v_hbm, vd, v_sem)):
        @pl.loop(0, keys // blk)
        def _(c):
            row = pl.multiple_of(c * (blk * kvl), blk * kvl)
            col = pl.multiple_of(c * blk, blk)
            cache_copy(src, held, sem, c).wait()
            stage[0:blk * kvl, :] = held[pl.ds(row, blk * kvl), :].astype(F32)
            for h in range(kvl):
                split_ref[h, pl.ds(col, blk), :] = stage[pl.ds(h, blk, stride=kvl), :].astype(BF16)

    valid = len_ref[0]
    per = group * hd // cr
    rows = group * tok

    def acc_copy(dest, src):
        return pltpu.make_async_remote_copy(
            src_ref=acc_send.at[pl.ds(pl.multiple_of(dest * cr, cr), cr), :],
            dst_ref=acc_rec.at[src], send_sem=a_ssem.at[dest], recv_sem=a_rsem.at[src],
            device_id=(dest, hm), device_id_type=MESH)

    def st_copy(dest, src):
        return pltpu.make_async_remote_copy(
            src_ref=st_send.at[(dest * cr) // hd],
            dst_ref=st_rec.at[src], send_sem=t_ssem.at[dest], recv_sem=t_rsem.at[src],
            device_id=(dest, hm), device_id_type=MESH)

    first = (me * cr) // (hd * group) + 1

    @pl.loop(0, kvl)
    def _(i):
        k = lax.rem(first + i, kvl)
        qq = qd[k]
        peaks = jnp.full((rows, 128), NEG, F32)
        for c in range(0, keys, blk):
            s = lax.dot_general(qq, kd[k, c:c + blk, :], (((1,), (1,)), ((), ())),
                                preferred_element_type=F32)
            pos = lax.broadcasted_iota(jnp.int32, (1, blk), 1) + c
            s = s + jnp.where(pos < valid, 0.0, NEG)
            s_scr[:, c:c + blk] = s
            for j in range(0, blk, 128):
                peaks = jnp.maximum(peaks, s[:, j:j + 128])
        peak = jnp.max(peaks, axis=1, keepdims=True)
        sums = jnp.zeros((rows, 128), F32)
        acc = jnp.zeros((rows, hd), F32)
        for c in range(0, keys, blk):
            w = jnp.exp2((s_scr[:, c:c + blk] - peak) * coef)
            for j in range(0, blk, 128):
                sums = sums + w[:, j:j + 128]
            acc = acc + jnp.dot(w.astype(BF16), vd[k, c:c + blk, :], preferred_element_type=F32)
        total = jnp.sum(sums, axis=1, keepdims=True)
        lane = lax.broadcasted_iota(jnp.int32, (rows, 128), 1)
        stats = jnp.where(lane == 0, peak, total).T
        low = acc.T.astype(BF16)
        for g in range(group):
            h = k * group + g
            acc_send[pl.ds(pl.multiple_of(h * hd, hd), hd), :] = low[:, g * tok:(g + 1) * tok]
            st_send[h] = stats[0:2, g * tok:(g + 1) * tok]

        @pl.when(i == 0)
        def _():
            pl.semaphore_wait(barrier, arrivals)

        for j in range(per):
            dest = k * per + j

            @pl.when(dest != me)
            def _():
                st_copy(dest, me).start()
                acc_copy(dest, me).start()

    acc_rec[me] = acc_send[pl.ds(pl.multiple_of(me * cr, cr), cr), :]
    st_rec[me] = st_send[(me * cr) // hd]

    @pl.loop(1, n)
    def _(d):
        src = lax.rem(me + d, n)
        st_copy(src, src).wait_recv()
        acc_copy(src, src).wait_recv()

    top = st_rec[0, 0:1, :]
    for b in range(1, n):
        top = jnp.maximum(top, st_rec[b, 0:1, :])
    whole = jnp.zeros((1, tok), F32)
    comb = jnp.zeros((cr, tok), F32)
    for b in range(n):
        f = jnp.exp2((st_rec[b, 0:1, :] - top) * coef)
        whole = whole + f * st_rec[b, 1:2, :]
        comb = comb + f * acc_rec[b].astype(F32)
    attn[pl.ds(pl.multiple_of(me * cr, cr), cr), :] = (comb / whole).astype(BF16)

    def g_copy(owner, dest):
        part = pl.ds(pl.multiple_of(owner * cr, cr), cr)
        return pltpu.make_async_remote_copy(
            src_ref=attn.at[part, :], dst_ref=attn.at[part, :],
            send_sem=g_ssem.at[dest], recv_sem=g_rsem.at[owner],
            device_id=(dest, hm), device_id_type=MESH)

    side = lax.rem(me, 2)
    partner = me + 1 - 2 * side
    turn = 1 - 2 * ((2 * me) // n)

    def peer(d):
        return lax.rem(me + 2 * d * turn + n, n)

    def f_copy(owner):
        part = pl.ds(pl.multiple_of(owner * cr, cr), cr)
        return pltpu.make_async_remote_copy(
            src_ref=attn.at[part, :], dst_ref=attn.at[part, :],
            send_sem=f_ssem.at[owner], recv_sem=g_rsem.at[owner],
            device_id=(partner, hm), device_id_type=MESH)

    @pl.loop(1, n // 2)
    def _(d):
        g_copy(me, peer(n // 2 - d)).start()
    g_copy(me, partner).start()

    cw.wait()

    @pl.loop(1, n // 2)
    def _(d):
        src = peer(d)
        g_copy(src, src).wait_recv()
        f_copy(src).start()
    g_copy(partner, partner).wait_recv()

    @pl.loop(1, n // 2)
    def _(d):
        src = lax.rem(partner + 2 * d, n)
        g_copy(src, src).wait_recv()

    proj = jnp.dot(win[...], attn[...], preferred_element_type=F32)
    psend[...] = proj.astype(BF16)

    def p_copy(owner, dest):
        part = psend.at[pl.ds(pl.multiple_of(dest * fq, fq), fq), :] if split else psend
        return pltpu.make_async_remote_copy(
            src_ref=part, dst_ref=prec.at[owner],
            send_sem=p_ssem.at[dest], recv_sem=p_rsem.at[owner],
            device_id=(me, dest), device_id_type=MESH)

    for d in range(1, hn):
        p_copy(hm, lax.rem(hm + d, hn)).start()
    if split:
        prec[hm] = psend[pl.ds(pl.multiple_of(hm * fq, fq), fq), :]
    else:
        prec[hm] = psend[...]
    for d in range(1, hn):
        src = lax.rem(hm + d, hn)
        p_copy(src, src).wait_recv()
    mine = prec[0].astype(F32)
    for b in range(1, hn):
        mine = mine + prec[b].astype(F32)

    def r_copy(owner, dest):
        part = pl.ds(pl.multiple_of(owner * fq, fq), fq)
        return pltpu.make_async_remote_copy(
            src_ref=pg.at[part, :], dst_ref=pg.at[part, :],
            send_sem=r_ssem.at[dest], recv_sem=r_rsem.at[owner],
            device_id=(me, dest), device_id_type=MESH)

    ss_send[...] = jnp.sum(mine * mine, axis=0, keepdims=True)
    members = total_dev if split else n
    mid = tid if split else me

    def s_copy(owner, dest):
        to = (dest // hn, lax.rem(dest, hn)) if split else (dest, hm)
        return pltpu.make_async_remote_copy(
            src_ref=ss_send, dst_ref=ss_rec.at[owner],
            send_sem=s_ssem.at[dest], recv_sem=s_rsem.at[owner],
            device_id=to, device_id_type=MESH)

    @pl.loop(1, members)
    def _(d):
        s_copy(mid, lax.rem(mid + d, members)).start()
    ss_rec[mid] = ss_send[...]

    if split:
        pg[pl.ds(pl.multiple_of(hm * fq, fq), fq), :] = mine.astype(BF16)
        for d in range(1, hn):
            r_copy(hm, lax.rem(hm + d, hn)).start()
        for d in range(1, hn):
            src = lax.rem(hm + d, hn)
            r_copy(src, src).wait_recv()
    else:
        pg[...] = mine.astype(BF16)

    @pl.loop(1, members)
    def _(d):
        src = lax.rem(mid + d, members)
        s_copy(src, src).wait_recv()

    square = jnp.sum(ss_rec[...], axis=0)
    factor = lax.rsqrt(square / (feat * n) + 1e-06)
    out_ref[...] = pg[...].astype(F32) * factor

    @pl.loop(1, n)
    def _(d):
        dest = lax.rem(me + d, n)
        st_copy(dest, me).wait_send()
        acc_copy(dest, me).wait_send()

    @pl.loop(1, n // 2)
    def _(d):
        dest = lax.rem(me + 2 * d, n)
        g_copy(me, dest).wait_send()
        f_copy(dest).wait_send()
    g_copy(me, partner).wait_send()
    for d in range(1, hn):
        dest = lax.rem(hm + d, hn)
        p_copy(hm, dest).wait_send()
        if split:
            r_copy(hm, dest).wait_send()

    @pl.loop(1, members)
    def _(d):
        s_copy(mid, lax.rem(mid + d, members)).wait_send()


def body(n, hn, query, key_cache, value_cache, lengths, out_weight, norm_gain):
    tok, heads, hd = query.shape
    keys, kvl, _ = key_cache.shape
    feat, width = out_weight.shape
    group = heads // kvl
    split = feat % (16 * hn) == 0
    blk = math.gcd(keys, 512)
    cr = width // n
    fq = feat // hn if split else feat
    members = n * hn if split else n
    cfg = (n, hn, keys, kvl, group, tok, hd, feat, split, blk)
    dma = pltpu.SemaphoreType.DMA
    hbm = pl.BlockSpec(memory_space=pl.ANY)
    scaled = pl.pallas_call(
        functools.partial(kernel, cfg),
        out_shape=jax.ShapeDtypeStruct((feat, tok), F32),
        in_specs=[hbm, hbm, hbm, pl.BlockSpec(memory_space=pltpu.SMEM), hbm],
        out_specs=pl.BlockSpec(memory_space=pltpu.VMEM),
        scratch_shapes=[
            pltpu.VMEM((tok * heads, hd), BF16),
            pltpu.VMEM((keys * kvl, hd), BF16),
            pltpu.VMEM((keys * kvl, hd), BF16),
            pltpu.VMEM((feat, width), BF16),
            pltpu.VMEM((max(blk * kvl, tok * heads), hd), F32),
            pltpu.VMEM((kvl, group * tok, hd), BF16),
            pltpu.VMEM((kvl, keys, hd), BF16),
            pltpu.VMEM((kvl, keys, hd), BF16),
            pltpu.VMEM((group * tok, keys), F32),
            pltpu.VMEM((width, tok), BF16),
            pltpu.VMEM((n, cr, tok), BF16),
            pltpu.VMEM((heads, 2, tok), F32),
            pltpu.VMEM((n, 2, tok), F32),
            pltpu.VMEM((width, tok), BF16),
            pltpu.VMEM((feat, tok), BF16),
            pltpu.VMEM((hn, fq, tok), BF16),
            pltpu.VMEM((feat, tok), BF16),
            pltpu.VMEM((1, tok), F32),
            pltpu.VMEM((members, 1, tok), F32),
            dma((2,)), dma((keys // blk,)), dma((keys // blk,)), dma((n,)), dma((n,)), dma((n,)), dma((n,)), dma((n,)), dma((n,)),
            dma((n,)), dma((hn,)), dma((hn,)), dma((hn,)), dma((hn,)), dma((members,)), dma((members,)),
        ],
        compiler_params=pltpu.CompilerParams(collective_id=0, has_side_effects=True),
    )(query.reshape(tok * heads, hd), key_cache.reshape(keys * kvl, hd),
      value_cache.reshape(keys * kvl, hd), lengths, out_weight)
    return (scaled * norm_gain[:, None]).astype(BF16).T


def solution(mesh):
    placed = (
        P(None, "head", None),
        P("seq", "head", None),
        P("seq", "head", None),
        P("seq"),
        P("seq", "head"),
        P("seq"),
    )
    return jax.shard_map(
        functools.partial(body, mesh.shape["seq"], mesh.shape["head"]),
        mesh=mesh, in_specs=placed, out_specs=P(None, "seq"), check_vma=False,
    )
```

```python
import functools
import math

import jax
import jax.numpy as jnp
from jax import lax
from jax.experimental import pallas as pl
from jax.experimental.pallas import tpu as pltpu
from jax.sharding import PartitionSpec as P

QPRE = 144
MESH = pl.DeviceIdType.MESH
BF16 = jnp.bfloat16
F32 = jnp.float32
NEG = -1e30


def kernel(cfg, q_hbm, k_hbm, v_hbm, len_ref, w_hbm, out_ref,
           qin, kin, vin, win, stage, qd, kd, vd, s_scr,
           acc_send, acc_rec, st_send, st_rec, attn, psend, prec, pg, ss_send, ss_rec,
           lsem, k_sem, v_sem, a_ssem, a_rsem, t_ssem, t_rsem, g_ssem, g_rsem, f_ssem, p_ssem, p_rsem,
           r_ssem, r_rsem, s_ssem, s_rsem):
    n, hn, keys, kvl, group, tok, hd, feat, split, blk = cfg
    heads = kvl * group
    width = heads * hd
    cr = width // n
    fq = feat // hn if split else feat
    me = lax.axis_index("seq")
    hm = lax.axis_index("head")
    tid = me * hn + hm
    total_dev = n * hn
    coef = float(QPRE) ** (-0.5) * math.log2(math.e)

    cq = pltpu.make_async_copy(q_hbm, qin, lsem.at[0])
    cw = pltpu.make_async_copy(w_hbm, win, lsem.at[1])

    def cache_copy(src, dst, sem, c):
        part = pl.ds(pl.multiple_of(c * (blk * kvl), blk * kvl), blk * kvl)
        return pltpu.make_async_copy(src.at[part, :], dst.at[part, :], sem.at[c])

    cq.start()
    for c in range(keys // blk):
        cache_copy(k_hbm, kin, k_sem, c).start()
    for c in range(keys // blk):
        cache_copy(v_hbm, vin, v_sem, c).start()
    cw.start()

    barrier = pltpu.get_barrier_semaphore()
    if split:
        @pl.loop(1, total_dev)
        def _(d):
            t = lax.rem(tid + d, total_dev)
            pl.semaphore_signal(barrier, inc=1, device_id=(t // hn, lax.rem(t, hn)), device_id_type=MESH)
        arrivals = total_dev - 1
    else:
        @pl.loop(1, n)
        def _(d):
            pl.semaphore_signal(barrier, inc=1, device_id=(lax.rem(me + d, n), hm), device_id_type=MESH)
        for d in range(1, hn):
            pl.semaphore_signal(barrier, inc=1, device_id=(me, lax.rem(hm + d, hn)), device_id_type=MESH)
        arrivals = n + hn - 2

    cq.wait()
    stage[0:tok * heads, :] = qin[...].astype(F32)
    for h in range(heads):
        qd[h // group, (h % group) * tok:(h % group + 1) * tok, :] = (
            stage[pl.ds(h, tok, stride=heads), :].astype(BF16))

    for held, src, split_ref, sem in ((kin, k_hbm, kd, k_sem), (vin, v_hbm, vd, v_sem)):
        @pl.loop(0, keys // blk, unroll=True)
        def _(c):
            row = pl.multiple_of(c * (blk * kvl), blk * kvl)
            col = pl.multiple_of(c * blk, blk)
            cache_copy(src, held, sem, c).wait()
            stage[0:blk * kvl, :] = held[pl.ds(row, blk * kvl), :].astype(F32)
            for h in range(kvl):
                split_ref[h, pl.ds(col, blk), :] = stage[pl.ds(h, blk, stride=kvl), :].astype(BF16)

    valid = len_ref[0]
    per = group * hd // cr
    rows = group * tok

    def acc_copy(dest, src):
        return pltpu.make_async_remote_copy(
            src_ref=acc_send.at[pl.ds(pl.multiple_of(dest * cr, cr), cr), :],
            dst_ref=acc_rec.at[src], send_sem=a_ssem.at[dest], recv_sem=a_rsem.at[src],
            device_id=(dest, hm), device_id_type=MESH)

    def st_copy(dest, src):
        return pltpu.make_async_remote_copy(
            src_ref=st_send.at[(dest * cr) // hd],
            dst_ref=st_rec.at[src], send_sem=t_ssem.at[dest], recv_sem=t_rsem.at[src],
            device_id=(dest, hm), device_id_type=MESH)

    first = (me * cr) // (hd * group) + 1

    @pl.loop(0, kvl, unroll=True)
    def _(i):
        k = lax.rem(first + i, kvl)
        qq = qd[k]
        peaks = jnp.full((rows, 128), NEG, F32)
        for c in range(0, keys, blk):
            s = lax.dot_general(qq, kd[k, c:c + blk, :], (((1,), (1,)), ((), ())),
                                preferred_element_type=F32)
            pos = lax.broadcasted_iota(jnp.int32, (1, blk), 1) + c
            s = s + jnp.where(pos < valid, 0.0, NEG)
            s_scr[:, c:c + blk] = s
            for j in range(0, blk, 128):
                peaks = jnp.maximum(peaks, s[:, j:j + 128])
        peak = jnp.max(peaks, axis=1, keepdims=True)
        sums = jnp.zeros((rows, 128), F32)
        acc = jnp.zeros((rows, hd), F32)
        for c in range(0, keys, blk):
            w = jnp.exp2((s_scr[:, c:c + blk] - peak) * coef)
            for j in range(0, blk, 128):
                sums = sums + w[:, j:j + 128]
            acc = acc + jnp.dot(w.astype(BF16), vd[k, c:c + blk, :], preferred_element_type=F32)
        total = jnp.sum(sums, axis=1, keepdims=True)
        lane = lax.broadcasted_iota(jnp.int32, (rows, 128), 1)
        stats = jnp.where(lane == 0, peak, total).T
        low = acc.T.astype(BF16)
        for g in range(group):
            h = k * group + g
            acc_send[pl.ds(pl.multiple_of(h * hd, hd), hd), :] = low[:, g * tok:(g + 1) * tok]
            st_send[h] = stats[0:2, g * tok:(g + 1) * tok]

        @pl.when(i == 0)
        def _():
            pl.semaphore_wait(barrier, arrivals)

        for j in range(per):
            dest = k * per + j

            @pl.when(dest != me)
            def _():
                st_copy(dest, me).start()
                acc_copy(dest, me).start()

    acc_rec[me] = acc_send[pl.ds(pl.multiple_of(me * cr, cr), cr), :]
    st_rec[me] = st_send[(me * cr) // hd]

    @pl.loop(1, n)
    def _(d):
        src = lax.rem(me + d, n)
        st_copy(src, src).wait_recv()
        acc_copy(src, src).wait_recv()

    top = st_rec[0, 0:1, :]
    for b in range(1, n):
        top = jnp.maximum(top, st_rec[b, 0:1, :])
    whole = jnp.zeros((1, tok), F32)
    comb = jnp.zeros((cr, tok), F32)
    for b in range(n):
        f = jnp.exp2((st_rec[b, 0:1, :] - top) * coef)
        whole = whole + f * st_rec[b, 1:2, :]
        comb = comb + f * acc_rec[b].astype(F32)
    attn[pl.ds(pl.multiple_of(me * cr, cr), cr), :] = (comb / whole).astype(BF16)

    def g_copy(owner, dest):
        part = pl.ds(pl.multiple_of(owner * cr, cr), cr)
        return pltpu.make_async_remote_copy(
            src_ref=attn.at[part, :], dst_ref=attn.at[part, :],
            send_sem=g_ssem.at[dest], recv_sem=g_rsem.at[owner],
            device_id=(dest, hm), device_id_type=MESH)

    side = lax.rem(me, 2)
    partner = me + 1 - 2 * side
    turn = 1 - 2 * ((2 * me) // n)

    def peer(d):
        return lax.rem(me + 2 * d * turn + n, n)

    def f_copy(owner):
        part = pl.ds(pl.multiple_of(owner * cr, cr), cr)
        return pltpu.make_async_remote_copy(
            src_ref=attn.at[part, :], dst_ref=attn.at[part, :],
            send_sem=f_ssem.at[owner], recv_sem=g_rsem.at[owner],
            device_id=(partner, hm), device_id_type=MESH)

    @pl.loop(1, n // 2)
    def _(d):
        g_copy(me, peer(n // 2 - d)).start()
    g_copy(me, partner).start()

    cw.wait()

    @pl.loop(1, n // 2)
    def _(d):
        src = peer(d)
        g_copy(src, src).wait_recv()
        f_copy(src).start()
    g_copy(partner, partner).wait_recv()

    @pl.loop(1, n // 2)
    def _(d):
        src = lax.rem(partner + 2 * d, n)
        g_copy(src, src).wait_recv()

    proj = jnp.dot(win[...], attn[...], preferred_element_type=F32)
    psend[...] = proj.astype(BF16)

    def p_copy(owner, dest):
        part = psend.at[pl.ds(pl.multiple_of(dest * fq, fq), fq), :] if split else psend
        return pltpu.make_async_remote_copy(
            src_ref=part, dst_ref=prec.at[owner],
            send_sem=p_ssem.at[dest], recv_sem=p_rsem.at[owner],
            device_id=(me, dest), device_id_type=MESH)

    for d in range(1, hn):
        p_copy(hm, lax.rem(hm + d, hn)).start()
    if split:
        prec[hm] = psend[pl.ds(pl.multiple_of(hm * fq, fq), fq), :]
    else:
        prec[hm] = psend[...]
    for d in range(1, hn):
        src = lax.rem(hm + d, hn)
        p_copy(src, src).wait_recv()
    mine = prec[0].astype(F32)
    for b in range(1, hn):
        mine = mine + prec[b].astype(F32)

    def r_copy(owner, dest):
        part = pl.ds(pl.multiple_of(owner * fq, fq), fq)
        return pltpu.make_async_remote_copy(
            src_ref=pg.at[part, :], dst_ref=pg.at[part, :],
            send_sem=r_ssem.at[dest], recv_sem=r_rsem.at[owner],
            device_id=(me, dest), device_id_type=MESH)

    ss_send[...] = jnp.sum(mine * mine, axis=0, keepdims=True)
    members = total_dev if split else n
    mid = tid if split else me

    def s_copy(owner, dest):
        to = (dest // hn, lax.rem(dest, hn)) if split else (dest, hm)
        return pltpu.make_async_remote_copy(
            src_ref=ss_send, dst_ref=ss_rec.at[owner],
            send_sem=s_ssem.at[dest], recv_sem=s_rsem.at[owner],
            device_id=to, device_id_type=MESH)

    @pl.loop(1, members)
    def _(d):
        s_copy(mid, lax.rem(mid + d, members)).start()
    ss_rec[mid] = ss_send[...]

    if split:
        pg[pl.ds(pl.multiple_of(hm * fq, fq), fq), :] = mine.astype(BF16)
        for d in range(1, hn):
            r_copy(hm, lax.rem(hm + d, hn)).start()
        for d in range(1, hn):
            src = lax.rem(hm + d, hn)
            r_copy(src, src).wait_recv()
    else:
        pg[...] = mine.astype(BF16)

    @pl.loop(1, members)
    def _(d):
        src = lax.rem(mid + d, members)
        s_copy(src, src).wait_recv()

    square = jnp.sum(ss_rec[...], axis=0)
    factor = lax.rsqrt(square / (feat * n) + 1e-06)
    out_ref[...] = pg[...].astype(F32) * factor

    @pl.loop(1, n)
    def _(d):
        dest = lax.rem(me + d, n)
        st_copy(dest, me).wait_send()
        acc_copy(dest, me).wait_send()

    @pl.loop(1, n // 2)
    def _(d):
        dest = lax.rem(me + 2 * d, n)
        g_copy(me, dest).wait_send()
        f_copy(dest).wait_send()
    g_copy(me, partner).wait_send()
    for d in range(1, hn):
        dest = lax.rem(hm + d, hn)
        p_copy(hm, dest).wait_send()
        if split:
            r_copy(hm, dest).wait_send()

    @pl.loop(1, members)
    def _(d):
        s_copy(mid, lax.rem(mid + d, members)).wait_send()


def body(n, hn, query, key_cache, value_cache, lengths, out_weight, norm_gain):
    tok, heads, hd = query.shape
    keys, kvl, _ = key_cache.shape
    feat, width = out_weight.shape
    group = heads // kvl
    split = feat % (16 * hn) == 0
    blk = math.gcd(keys, 512)
    cr = width // n
    fq = feat // hn if split else feat
    members = n * hn if split else n
    cfg = (n, hn, keys, kvl, group, tok, hd, feat, split, blk)
    dma = pltpu.SemaphoreType.DMA
    hbm = pl.BlockSpec(memory_space=pl.ANY)
    scaled = pl.pallas_call(
        functools.partial(kernel, cfg),
        out_shape=jax.ShapeDtypeStruct((feat, tok), F32),
        in_specs=[hbm, hbm, hbm, pl.BlockSpec(memory_space=pltpu.SMEM), hbm],
        out_specs=pl.BlockSpec(memory_space=pltpu.VMEM),
        scratch_shapes=[
            pltpu.VMEM((tok * heads, hd), BF16),
            pltpu.VMEM((keys * kvl, hd), BF16),
            pltpu.VMEM((keys * kvl, hd), BF16),
            pltpu.VMEM((feat, width), BF16),
            pltpu.VMEM((max(blk * kvl, tok * heads), hd), F32),
            pltpu.VMEM((kvl, group * tok, hd), BF16),
            pltpu.VMEM((kvl, keys, hd), BF16),
            pltpu.VMEM((kvl, keys, hd), BF16),
            pltpu.VMEM((group * tok, keys), F32),
            pltpu.VMEM((width, tok), BF16),
            pltpu.VMEM((n, cr, tok), BF16),
            pltpu.VMEM((heads, 2, tok), F32),
            pltpu.VMEM((n, 2, tok), F32),
            pltpu.VMEM((width, tok), BF16),
            pltpu.VMEM((feat, tok), BF16),
            pltpu.VMEM((hn, fq, tok), BF16),
            pltpu.VMEM((feat, tok), BF16),
            pltpu.VMEM((1, tok), F32),
            pltpu.VMEM((members, 1, tok), F32),
            dma((2,)), dma((keys // blk,)), dma((keys // blk,)), dma((n,)), dma((n,)), dma((n,)), dma((n,)), dma((n,)), dma((n,)),
            dma((n,)), dma((hn,)), dma((hn,)), dma((hn,)), dma((hn,)), dma((members,)), dma((members,)),
        ],
        compiler_params=pltpu.CompilerParams(collective_id=0, has_side_effects=True),
    )(query.reshape(tok * heads, hd), key_cache.reshape(keys * kvl, hd),
      value_cache.reshape(keys * kvl, hd), lengths, out_weight)
    return (scaled * norm_gain[:, None]).astype(BF16).T


def solution(mesh):
    placed = (
        P(None, "head", None),
        P("seq", "head", None),
        P("seq", "head", None),
        P("seq"),
        P("seq", "head"),
        P("seq"),
    )
    return jax.shard_map(
        functools.partial(body, mesh.shape["seq"], mesh.shape["head"]),
        mesh=mesh, in_specs=placed, out_specs=P(None, "seq"), check_vma=False,
    )
```
